32 devices in a mesh: probe: 4 (over x, core), fsdp: 8 (over z, y).
Axes of the slice: x: 2, y: 2, z: 4, core: 2. Of those that a mesh axis runs over, the one named last changes fastest.
Arguments:
- hidden: bfloat16 [16384, 2048], P(('probe', 'fsdp')), may hold values from -6 to 6
- norm_gain: bfloat16 [2048], replicated, may hold values from 0.5 to 1.5
- query_weight: bfloat16 [2048, 2048], P('fsdp'), may hold values from -1 to 1
- key_weight: bfloat16 [2048, 512], P('fsdp'), may hold values from -16 to 16
- value_weight: bfloat16 [2048, 512], P('fsdp'), may hold values from -0.125 to 0.125
- output_weight: bfloat16 [2048, 2048], P('fsdp'), may hold values from -0.125 to 0.125
- probe_seed: int32 [4], P('probe'), may hold values from 0 to 1073741823
Outputs:
- curvature_value: float32 [2048, 512], P('fsdp', 'probe')
- curvature_output: float32 [2048, 2048], P('fsdp', 'probe')
The draws below stay inside these ranges and needn't reach their ends.
All inputs are finite; a program needn't handle non-finite values.
Results may differ from the reference program's by a relative error of at most 0.024.
Values may be sent and summed in bfloat16 or wider, within the bound.
A program may use at most 128 MiB of HBM per device.

```python
import jax
import jax.numpy as jnp
from jax import lax

D = 2048
HEADS = 16
KV_HEADS = 4
HEAD_DIM = 128
SEQ = 256
TOK_DEV = 512
QW = 2048
KW = 512
TOKENS = 16384
N_PROBE = 4
N_FSDP = 8


def query_base(key):
    normals = jax.random.normal(jax.random.fold_in(key, 7101), (D, HEADS * HEAD_DIM), jnp.float32)
    return jnp.clip(normals, -6.0, 6.0) * D ** (-0.5)


def draw_query_weight(key, part):
    return query_base(key).astype(jnp.bfloat16)


def draw_key_weight(key, part):
    normals = jax.random.normal(jax.random.fold_in(key, 7102), (D, KV_HEADS * HEAD_DIM), jnp.float32)
    noise_part = jnp.clip(normals, -6.0, 6.0) * D ** (-0.5)
    return noise_part.astype(jnp.bfloat16)


def touch_ends(entries, own_key, least, largest):
    longest = entries.shape.index(max(entries.shape))
    spots = []
    for shift in (0, 1):
        where = [jax.random.randint(jax.random.fold_in(own_key, axis), (), 0, length) for axis, length in enumerate(entries.shape)]
        where[longest] = (where[longest] + shift) % entries.shape[longest]
        spots.append(tuple(where))
    return entries.at[spots[0]].set(least).at[spots[1]].set(largest)


def block_scale(stream_key, extent, split, smallest, largest):
    factor_of = 1.0
    for axis_at, blocks in split:
        draws = jax.random.uniform(jax.random.fold_in(jax.random.fold_in(stream_key, 6), axis_at), (blocks,), jnp.float32, smallest / len(split), largest / len(split))
        factor_of = factor_of * jnp.repeat(jnp.exp(draws), extent[axis_at] // blocks).reshape((-1,) + (1,) * (len(extent) - 1 - axis_at))
    return factor_of


def gaussian(stream_key, shape, scale, bound, split=(), kind=jnp.bfloat16):
    factor_of = block_scale(stream_key, shape, split, -0.22, 0.18) if split else 1.0
    values = jax.random.normal(stream_key, shape, jnp.float32) * scale * factor_of
    return jnp.minimum(jnp.maximum(values, -bound), bound).astype(kind)


def setup_inputs(seed: int = 0) -> dict:
    seeds = jax.random.split(jax.random.key(seed), 8)
    return {
        "hidden": gaussian(seeds[0], (TOKENS, D), 1.0, 6.0, ((0, 32),)),
        "norm_gain": jnp.clip(1.0 + 0.1 * jax.random.normal(seeds[1], (D,), jnp.float32), 0.5, 1.5).astype(jnp.bfloat16),
        "query_weight": draw_query_weight(jax.random.fold_in(seeds[7], 71), 0),
        "key_weight": draw_key_weight(jax.random.fold_in(seeds[7], 71), 0),
        "value_weight": gaussian(seeds[4], (D, KW), D ** -0.5, 0.125, ((0, 8),)),
        "output_weight": gaussian(seeds[5], (QW, D), QW ** -0.5, 0.125, ((0, 8),)),
        "probe_seed": touch_ends(jax.random.randint(seeds[6], (N_PROBE,), 0, 1073741824), jax.random.fold_in(seeds[6], 1), 0, 1073741823).astype(jnp.int32),
    }


norm_eps = 1e-05
rope_base = 500000.0

def sign_table(seed_value, matrix_code, row_total, column_total):
    row_index = lax.broadcasted_iota(jnp.int32, (row_total, column_total), 0)
    column_index = lax.broadcasted_iota(jnp.int32, (row_total, column_total), 1)
    hashed = (row_index * column_total + column_index) * 747796405 + (seed_value * 1664525 + matrix_code * 374761393)
    hashed = hashed ^ lax.shift_right_logical(hashed, jnp.int32(15))
    hashed = hashed * 668265261
    hashed = hashed ^ lax.shift_right_logical(hashed, jnp.int32(13))
    hashed = hashed * 1274126177
    hashed = hashed ^ lax.shift_right_logical(hashed, jnp.int32(16))
    return jnp.where(hashed & 1 == 1, 1.0, -1.0).astype(jnp.bfloat16)

def normalize(rows_in, gain_row):
    values = rows_in.astype(jnp.float32)
    inverse = lax.rsqrt(lax.optimization_barrier(jnp.mean(values * values, axis=1, keepdims=True)) + norm_eps)
    return (values * inverse * gain_row.astype(jnp.float32)[None, :]).astype(jnp.bfloat16)

def rotate(projected, head_count):
    row_count = projected.shape[0]
    columns = projected.shape[1]
    head_size = columns // head_count
    half_dim = head_size // 2
    position = (lax.broadcasted_iota(jnp.int32, (row_count, 1), 0) % SEQ).astype(jnp.float32)
    exponent = lax.broadcasted_iota(jnp.int32, (1, half_dim), 1).astype(jnp.float32) * (-2.0 / head_size)
    frequency = jnp.power(jnp.float32(rope_base), exponent)
    angles = position * frequency
    cosine = jnp.cos(angles)[:, None, :]
    sine_part = jnp.sin(angles)[:, None, :]
    shaped = projected.reshape(row_count, head_count, head_size)
    leading = shaped[:, :, :half_dim]
    trailing = shaped[:, :, half_dim:]
    turned = jnp.concatenate([leading * cosine - trailing * sine_part, trailing * cosine + leading * sine_part], axis=2)
    return turned.reshape(row_count, columns).astype(jnp.bfloat16)

def attend(query_rows, key_rows):
    row_count = query_rows.shape[0]
    key_heads = key_rows.shape[1] // HEAD_DIM
    group_size = query_rows.shape[1] // key_rows.shape[1]
    sequences = row_count // SEQ
    grouped_query = query_rows.reshape(sequences, SEQ, key_heads, group_size, HEAD_DIM).astype(jnp.float32)
    grouped_key = key_rows.reshape(sequences, SEQ, key_heads, HEAD_DIM).astype(jnp.float32)
    scores = jnp.einsum('bqkgd,bskd->bkgqs', grouped_query, grouped_key) * HEAD_DIM ** (-0.5)
    causal_mask = lax.broadcasted_iota(jnp.int32, (SEQ, SEQ), 0) >= lax.broadcasted_iota(jnp.int32, (SEQ, SEQ), 1)
    scores = jnp.where(causal_mask, scores, -1e+30)
    highest = lax.optimization_barrier(jnp.max(scores, axis=4, keepdims=True))
    raised = jnp.exp(scores - highest)
    return (raised / lax.optimization_barrier(jnp.sum(raised, axis=4, keepdims=True))).astype(jnp.bfloat16)

def mix_values(attention, value_rows):
    sequences = attention.shape[0]
    key_heads = attention.shape[1]
    group_size = attention.shape[2]
    grouped_value = value_rows.reshape(sequences, SEQ, key_heads, HEAD_DIM).astype(jnp.float32)
    combined = jnp.einsum('bkgqs,bskd->bqkgd', attention.astype(jnp.float32), grouped_value)
    return combined.reshape(sequences * SEQ, key_heads * group_size * HEAD_DIM)

def spread_back(attention, upstream):
    sequences = attention.shape[0]
    key_heads = attention.shape[1]
    group_size = attention.shape[2]
    grouped_upstream = upstream.reshape(sequences, SEQ, key_heads, group_size, HEAD_DIM).astype(jnp.float32)
    spread = jnp.einsum('bkgqs,bqkgd->bskd', attention.astype(jnp.float32), grouped_upstream)
    return spread.reshape(sequences * SEQ, key_heads * HEAD_DIM)

def device_terms(rows_in, norm_gain, query_weight, key_weight, value_weight, output_weight, seed_value):
    normed = normalize(rows_in, norm_gain)
    query_rows = rotate(jnp.dot(normed, query_weight, preferred_element_type=jnp.float32), HEADS)
    key_rows = rotate(jnp.dot(normed, key_weight, preferred_element_type=jnp.float32), KV_HEADS)
    value_rows = jnp.dot(normed, value_weight, preferred_element_type=jnp.float32).astype(jnp.bfloat16)
    attention = attend(query_rows, key_rows)
    context = mix_values(attention, value_rows).astype(jnp.bfloat16)
    signs_value = sign_table(seed_value, 0, D, KW)
    signs_out = sign_table(seed_value, 1, QW, D)
    tangent_value = (jnp.dot(normed, signs_value, preferred_element_type=jnp.float32) * D ** (-0.5)).astype(jnp.bfloat16)
    tangent_context = mix_values(attention, tangent_value).astype(jnp.bfloat16)
    forward_part = jnp.dot(tangent_context, output_weight, preferred_element_type=jnp.float32)
    probe_part = jnp.dot(context, signs_out, preferred_element_type=jnp.float32) * QW ** (-0.5)
    cotangent = (forward_part + probe_part).astype(jnp.bfloat16)
    back_context = jnp.dot(cotangent, output_weight.T, preferred_element_type=jnp.float32).astype(jnp.bfloat16)
    back_value = spread_back(attention, back_context).astype(jnp.bfloat16)
    term_value = jnp.dot(normed.T, back_value, preferred_element_type=jnp.float32)
    term_out = jnp.dot(context.T, cotangent, preferred_element_type=jnp.float32)
    return (term_value, term_out)

def reference(hidden, norm_gain, query_weight, key_weight, value_weight, output_weight, probe_seed):
    blocks = N_PROBE * N_FSDP

    def one_block(totals, block_index):
        rows_in = lax.dynamic_slice_in_dim(hidden, block_index * TOK_DEV, TOK_DEV, 0)
        seed_value = probe_seed[block_index // N_FSDP]
        term_value, term_out = device_terms(rows_in, norm_gain, query_weight, key_weight, value_weight, output_weight, seed_value)
        rounded_value = lax.optimization_barrier(term_value.astype(jnp.bfloat16))
        rounded_out = lax.optimization_barrier(term_out.astype(jnp.bfloat16))
        return ((totals[0] + rounded_value.astype(jnp.float32), totals[1] + rounded_out.astype(jnp.float32)), None)
    starting = (jnp.zeros((D, KW), jnp.float32), jnp.zeros((QW, D), jnp.float32))
    totals, unused = lax.scan(one_block, starting, jnp.arange(blocks, dtype=jnp.int32))
    return (totals[0], totals[1])
```

```python
import functools

import jax
import jax.numpy as jnp
from jax import lax
from jax.experimental import pallas as pl
from jax.experimental.pallas import tpu as pltpu
from jax.sharding import PartitionSpec as P

HEAD_DIM = 128
SEQ = 256


norm_eps = 1e-05
rope_base = 500000.0


def sign_table(seed_value, matrix_code, row_total, column_total):
    row_index = lax.broadcasted_iota(jnp.int32, (row_total, column_total), 0)
    column_index = lax.broadcasted_iota(jnp.int32, (row_total, column_total), 1)
    hashed = (row_index * column_total + column_index) * 747796405 + (
        seed_value * 1664525 + matrix_code * 374761393
    )
    hashed = hashed ^ lax.shift_right_logical(hashed, jnp.int32(15))
    hashed = hashed * 668265261
    hashed = hashed ^ lax.shift_right_logical(hashed, jnp.int32(13))
    hashed = hashed * 1274126177
    hashed = hashed ^ lax.shift_right_logical(hashed, jnp.int32(16))
    return jnp.where(hashed & 1 == 1, 1.0, -1.0).astype(jnp.bfloat16)


def normalize(rows_in, gain_row):
    values = rows_in.astype(jnp.float32)
    inverse = lax.rsqrt(jnp.mean(values * values, axis=1, keepdims=True) + norm_eps)
    return (values * inverse * gain_row.astype(jnp.float32)[None, :]).astype(jnp.bfloat16)


def turn_tables(head_size):
    half_dim = head_size // 2
    position = lax.broadcasted_iota(jnp.int32, (SEQ, 1), 0).astype(jnp.float32)
    exponent = lax.broadcasted_iota(jnp.int32, (1, half_dim), 1).astype(jnp.float32) * (
        -2.0 / head_size
    )
    angles = position * jnp.power(jnp.float32(rope_base), exponent)
    cosine = jnp.cos(angles)
    sine = jnp.sin(angles)
    return (
        jnp.concatenate([cosine, cosine], axis=1),
        jnp.concatenate([-sine, sine], axis=1),
    )


def attend_kernel(blocks, q_part, k_part, place_ref, *refs):
    raws = refs[:blocks]
    tangent_ref, cos_ref, sin_ref, context_ref, moved_ref, weight_ref = refs[blocks:]
    cosine = cos_ref[...]
    sine = sin_ref[...]
    group = q_part // k_part
    half = HEAD_DIM // 2
    mask = lax.broadcasted_iota(jnp.int32, (SEQ, SEQ), 0) >= lax.broadcasted_iota(
        jnp.int32, (SEQ, SEQ), 1
    )

    def turned(rows):
        swapped = jnp.concatenate([rows[:, half:], rows[:, :half]], axis=1)
        return (rows * cosine + swapped * sine).astype(jnp.bfloat16)

    for index in range(blocks):
        raw = raws[index]
        place = place_ref[0] ^ index
        for kv in range(k_part // HEAD_DIM):
            low = q_part + kv * HEAD_DIM
            key = turned(raw[:, low : low + HEAD_DIM])
            low = low + k_part
            value = raw[:, low : low + HEAD_DIM].astype(jnp.bfloat16)
            start = pl.multiple_of(place * k_part + kv * HEAD_DIM, HEAD_DIM)
            both = jnp.concatenate([value, tangent_ref[:, pl.ds(start, HEAD_DIM)]], axis=1)
            for member in range(group):
                head = kv * group + member
                query = turned(raw[:, head * HEAD_DIM : (head + 1) * HEAD_DIM])
                scores = lax.dot_general(
                    query, key, (((1,), (1,)), ((), ())), preferred_element_type=jnp.float32
                ) * HEAD_DIM ** (-0.5)
                scores = jnp.where(mask, scores, -1e30)
                raised = jnp.exp(scores - jnp.max(scores, axis=1, keepdims=True))
                weight = (raised / jnp.sum(raised, axis=1, keepdims=True)).astype(jnp.bfloat16)
                weight_ref[0, place * (q_part // HEAD_DIM) + head] = weight
                mixed = jnp.dot(weight, both, preferred_element_type=jnp.float32).astype(
                    jnp.bfloat16
                )
                start = pl.multiple_of(place * q_part + head * HEAD_DIM, HEAD_DIM)
                context_ref[:, pl.ds(start, HEAD_DIM)] = mixed[:, :HEAD_DIM]
                moved_ref[:, pl.ds(start, HEAD_DIM)] = mixed[:, HEAD_DIM:]


def attend(place, raws, tangent_value, q_part, k_part):
    rows = tangent_value.shape[0]
    blocks = len(raws)
    width = q_part * blocks
    heads = width // HEAD_DIM
    sequences = rows // SEQ
    cosine, sine = turn_tables(HEAD_DIM)
    by_sequence = lambda columns: pl.BlockSpec((SEQ, columns), lambda i: (i, 0))
    fixed = pl.BlockSpec((SEQ, HEAD_DIM), lambda i: (0, 0))
    return pl.pallas_call(
        functools.partial(attend_kernel, blocks, q_part, k_part),
        grid=(sequences,),
        in_specs=[pl.BlockSpec(memory_space=pltpu.SMEM)]
        + [by_sequence(raw.shape[1]) for raw in raws]
        + [by_sequence(tangent_value.shape[1]), fixed, fixed],
        out_specs=[
            by_sequence(width),
            by_sequence(width),
            pl.BlockSpec((1, heads, SEQ, SEQ), lambda i: (i, 0, 0, 0)),
        ],
        out_shape=[
            jax.ShapeDtypeStruct((rows, width), jnp.bfloat16),
            jax.ShapeDtypeStruct((rows, width), jnp.bfloat16),
            jax.ShapeDtypeStruct((sequences, heads, SEQ, SEQ), jnp.bfloat16),
        ],
        cost_estimate=pl.CostEstimate(
            flops=6 * rows * SEQ * width,
            bytes_accessed=16 * rows * width,
            transcendentals=rows * SEQ * heads,
        ),
    )(place.reshape(1).astype(jnp.int32), *raws, tangent_value, cosine, sine)


def spread_kernel(key_heads, group, weight_ref, upstream_ref, spread_ref):
    for kv in range(key_heads):
        total = jnp.zeros((SEQ, HEAD_DIM), jnp.float32)
        for member in range(group):
            head = kv * group + member
            total = total + lax.dot_general(
                weight_ref[0, head],
                upstream_ref[:, head * HEAD_DIM : (head + 1) * HEAD_DIM],
                (((0,), (0,)), ((), ())),
                preferred_element_type=jnp.float32,
            )
        spread_ref[:, kv * HEAD_DIM : (kv + 1) * HEAD_DIM] = total.astype(jnp.bfloat16)


def spread_back(attention, upstream, key_heads):
    sequences, heads = attention.shape[:2]
    rows, width = upstream.shape
    return pl.pallas_call(
        functools.partial(spread_kernel, key_heads, heads // key_heads),
        grid=(sequences,),
        in_specs=[
            pl.BlockSpec((1, heads, SEQ, SEQ), lambda i: (i, 0, 0, 0)),
            pl.BlockSpec((SEQ, width), lambda i: (i, 0)),
        ],
        out_specs=pl.BlockSpec((SEQ, key_heads * HEAD_DIM), lambda i: (i, 0)),
        out_shape=jax.ShapeDtypeStruct((rows, key_heads * HEAD_DIM), jnp.bfloat16),
        cost_estimate=pl.CostEstimate(
            flops=2 * rows * SEQ * width,
            bytes_accessed=6 * rows * width,
            transcendentals=0,
        ),
    )(attention, upstream)


def swap(block, axis, bit):
    pairs = [(index, index ^ bit) for index in range(lax.axis_size(axis))]
    return lax.ppermute(block, axis, pairs)


def axis_bits(axis):
    size = lax.axis_size(axis)
    bits = []
    bit = 1
    while bit < size:
        bits.append(bit)
        bit *= 2
    return bits


def gather_rows(piece):
    whole = piece[None]
    for bit in reversed(axis_bits("fsdp")):
        whole = jnp.concatenate([whole, swap(whole, "fsdp", bit)], axis=0)
    return whole


def order_rows():
    bits = list(reversed(axis_bits("fsdp")))
    order = [0]
    for bit in bits:
        order = order + [place ^ bit for place in order]
    return order


def reorder_by(rows_in, me, order):
    width = rows_in.shape[1] // len(order)
    return jnp.concatenate(
        [lax.dynamic_slice_in_dim(rows_in, (me ^ place) * width, width, 1) for place in order],
        axis=1,
    )


def column_piece(weight, index, parts):
    width = weight.shape[1] // parts
    return lax.dynamic_slice_in_dim(weight, index * width, width, 1)


def place_columns(pieces, indices, total):
    width = pieces[0].shape[1]
    whole = jnp.zeros((pieces[0].shape[0], width * total), pieces[0].dtype)
    for piece, index in zip(pieces, indices):
        whole = lax.dynamic_update_slice_in_dim(whole, piece, index * width, 1)
    return whole


def add_pair(left, right):
    return (left.astype(jnp.float32) + right.astype(jnp.float32)).astype(jnp.bfloat16)


def fold_rows(held, me, bits):
    for bit in bits:
        low = (me // bit) % 2
        sent, kept = [], []
        for array in held:
            split = array.reshape((array.shape[0] // 2, 2) + array.shape[1:])
            sent.append(lax.dynamic_index_in_dim(split, 1 - low, 1, keepdims=False))
            kept.append(lax.dynamic_index_in_dim(split, low, 1, keepdims=False))
        held = [add_pair(k, swap(s, "fsdp", bit)) for k, s in zip(kept, sent)]
    return held


def scatter_sum(terms, probe_first, fs):
    count = lax.axis_size("fsdp")
    bits = axis_bits("fsdp")
    held = [term.reshape(count, term.shape[0] // count, term.shape[1]) for term in terms]
    probe_bits = axis_bits("probe")
    held = [
        add_pair(held[index], swap(held[index ^ 1], "probe", 1))
        for index in range(0, len(held), 2)
    ]
    if probe_first:
        steps = [("probe", 0)] + [("fsdp", bit) for bit in bits]
    else:
        steps = [("fsdp", bits[0]), ("probe", 0)] + [("fsdp", bit) for bit in bits[1:]]
    for axis, bit in steps:
        if axis == "fsdp":
            held = fold_rows(held, fs, [bit])
        else:
            for probe_bit in probe_bits[1:]:
                held = [
                    add_pair(held[index], swap(held[index + 1], "probe", probe_bit))
                    for index in range(0, len(held), 2)
                ]
    return held[0][0].astype(jnp.float32)


def body(hidden, norm_gain, query_weight, key_weight, value_weight, output_weight, probe_seed):
    seed_value = probe_seed[0]
    model_width = hidden.shape[1]
    query_width = query_weight.shape[1]
    key_width = key_weight.shape[1]
    key_heads = key_width // HEAD_DIM
    probes = lax.axis_size("probe")
    shards = lax.axis_size("fsdp")
    pr = lax.axis_index("probe")
    fs = lax.axis_index("fsdp")
    core = pr % 2
    contract_rows = (((0,), (0,)), ((), ()))
    contract_columns = (((1,), (1,)), ((), ()))

    joint = jnp.concatenate(
        [column_piece(w, pr, probes) for w in (query_weight, key_weight, value_weight)], axis=1
    )
    joint = gather_rows(joint)
    order = order_rows()
    joint = joint.reshape(model_width, joint.shape[2])
    joint_blocks = {0: joint}
    for bit in axis_bits("probe")[1:]:
        for index in list(joint_blocks):
            joint_blocks[index ^ bit] = swap(joint_blocks[index], "probe", bit)
    for index in list(joint_blocks):
        joint_blocks[index ^ 1] = swap(joint_blocks[index], "probe", 1)

    out_piece = gather_rows(column_piece(output_weight, core, 2))
    out_piece = out_piece.reshape(query_width, out_piece.shape[2])
    out_blocks = [out_piece, swap(out_piece, "probe", 1)]

    normed = normalize(hidden, norm_gain)
    signs_value = sign_table(seed_value, 0, model_width, key_width)
    signs_out = sign_table(seed_value, 1, query_width, model_width)
    tangent_value = (
        jnp.dot(normed, signs_value, preferred_element_type=jnp.float32) * model_width ** (-0.5)
    ).astype(jnp.bfloat16)

    ordered = reorder_by(normed, fs, order)
    q_part = query_width // probes
    k_part = key_width // probes
    raws = [
        jnp.dot(ordered, joint_blocks[index], preferred_element_type=jnp.float32)
        for index in sorted(joint_blocks)
    ]
    context, tangent_context, attention = attend(pr, raws, tangent_value, q_part, k_part)
    probe_part = jnp.dot(context, signs_out, preferred_element_type=jnp.float32) * query_width ** (
        -0.5
    )
    ordered_tangent = reorder_by(tangent_context, fs, order)
    half = model_width // 2
    cot_pieces = []
    for index in range(2):
        forward_part = jnp.dot(
            ordered_tangent, out_blocks[index], preferred_element_type=jnp.float32
        )
        mine = lax.dynamic_slice_in_dim(probe_part, (core ^ index) * half, half, 1)
        cot_pieces.append((forward_part + mine).astype(jnp.bfloat16))
    cotangent = place_columns(cot_pieces, [core, core ^ 1], 2)

    chunk = model_width // probes
    out_terms = []
    for index in range(probes):
        columns = lax.dynamic_slice_in_dim(cotangent, (pr ^ index) * chunk, chunk, 1)
        out_terms.append(
            lax.dot_general(
                context, columns, contract_rows, preferred_element_type=jnp.float32
            ).astype(jnp.bfloat16)
        )
    curvature_output = jnp.concatenate(
        [
            scatter_sum([term[:, : chunk // 2] for term in out_terms], True, fs),
            scatter_sum([term[:, chunk // 2 :] for term in out_terms], False, fs),
        ],
        axis=1,
    )

    back_context = sum(
        lax.dot_general(
            cot_pieces[index],
            out_blocks[index],
            contract_columns,
            preferred_element_type=jnp.float32,
        )
        for index in range(2)
    ).astype(jnp.bfloat16)
    width = query_width // shards
    back_natural = unorder(back_context, fs, order, width)
    back_value = spread_back(attention, back_natural, key_heads)
    chunk = key_width // probes
    value_terms = []
    for index in range(probes):
        columns = lax.dynamic_slice_in_dim(back_value, (pr ^ index) * chunk, chunk, 1)
        value_terms.append(
            lax.dot_general(
                normed, columns, contract_rows, preferred_element_type=jnp.float32
            ).astype(jnp.bfloat16)
        )
    curvature_value = scatter_sum(value_terms, True, fs)
    return (curvature_value, curvature_output)


def unorder(rows_in, me, order, width):
    whole = jnp.zeros_like(rows_in)
    for index, place in enumerate(order):
        piece = rows_in[:, index * width : (index + 1) * width]
        whole = lax.dynamic_update_slice_in_dim(whole, piece, (me ^ place) * width, 1)
    return whole


def solution(mesh):
    return jax.shard_map(
        body,
        mesh=mesh,
        in_specs=(
            P(("probe", "fsdp"), None),
            P(),
            P("fsdp", None),
            P("fsdp", None),
            P("fsdp", None),
            P("fsdp", None),
            P("probe"),
        ),
        out_specs=(P("fsdp", "probe"), P("fsdp", "probe")),
        check_vma=False,
    )
```
